8 devices in a mesh: row: 4 (over z, y, x), col: 2 (over core).
Axes of the slice: x: 2, y: 2, z: 1, core: 2. Of those that a mesh axis runs over, the one named last changes fastest.
Arguments:
- w_in: float32 [4, 2, 2, 1024, 4096], P('row', 'col')
- w_out: float32 [4, 2, 2, 4096, 1024], P('row', 'col')
- inputs: bfloat16 [4, 2, 4, 2048, 1024], P('row', 'col')
- targets: bfloat16 [4, 2, 4, 2048, 1024], P('row', 'col')
Outputs:
- output 1: float32 [4, 2, 2, 1024, 4096], P('row', 'col')
- output 2: float32 [4, 2, 2, 4096, 1024], P('row', 'col')
All inputs are finite; a program needn't handle non-finite values.
Results may differ from the reference program's by a relative error of at most 0.001.
Values are sent between devices in bfloat16 or wider.
A program may use at most 1 GiB of HBM per device.

```python
import jax
import jax.numpy as jnp
from jax import lax

ROWS = 4
COLS = 2
LAYERS = 2
D = 1024
FF = 4096
BATCH = 2048
WINDOWS = 2

STEPS = 2 * WINDOWS
LEARN_RATE = 0.8 / LAYERS
EPS = 1e-6
INV_SQRT2 = 0.7071067811865476
INV_SQRT_2PI = 0.3989422804014327
SPREAD = 0.5
TARGET_SHIFT = 2.0


def setup_inputs(seed: int = 0) -> dict:
    key_list = jax.random.split(jax.random.key(seed), 8)
    norm_scale = (1.0 + SPREAD * SPREAD) ** -0.5
    shape_in = (ROWS, COLS, LAYERS, D, FF)
    shape_out = (ROWS, COLS, LAYERS, FF, D)
    data_shape = (ROWS, COLS, STEPS, BATCH, D)
    base_in = jax.random.normal(key_list[0], (LAYERS, D, FF), jnp.float32)
    base_out = jax.random.normal(key_list[1], (LAYERS, FF, D), jnp.float32)
    w_in = (base_in + SPREAD * jax.random.normal(key_list[2], shape_in, jnp.float32)) * (norm_scale * D ** -0.5)
    w_out = (base_out + SPREAD * jax.random.normal(key_list[3], shape_out, jnp.float32)) * (norm_scale * FF ** -0.5)
    shift_in = jax.random.normal(key_list[4], (ROWS, COLS, 1, 1, D), jnp.float32)
    shift_tgt = TARGET_SHIFT * jax.random.normal(key_list[5], (ROWS, COLS, 1, 1, D), jnp.float32)
    inputs = (jax.random.normal(key_list[6], data_shape, jnp.float32) + shift_in).astype(jnp.bfloat16)
    targets = (jax.random.normal(key_list[7], data_shape, jnp.float32) + shift_tgt).astype(jnp.bfloat16)
    return {"w_in": w_in, "w_out": w_out, "inputs": inputs, "targets": targets}


def rms_norm(rows):
    return rows * lax.rsqrt(jnp.mean(rows * rows, axis=-1, keepdims=True) + EPS)


def rms_back(rows, grad_norm):
    inv_rms = lax.rsqrt(jnp.mean(rows * rows, axis=-1, keepdims=True) + EPS)
    row_dot = jnp.mean(rows * grad_norm, axis=-1, keepdims=True)
    return inv_rms * grad_norm - rows * (inv_rms * inv_rms * inv_rms) * row_dot


def gelu_exact(pre_act):
    return 0.5 * pre_act * (1.0 + lax.erf(pre_act * INV_SQRT2))


def gelu_slope(pre_act):
    return 0.5 * (1.0 + lax.erf(pre_act * INV_SQRT2)) + pre_act * jnp.exp(-0.5 * pre_act * pre_act) * INV_SQRT_2PI


def device_grads(w_in, w_out, rows_in, rows_tgt):
    hidden = rows_in
    saved_acts = []
    for layer_idx in range(LAYERS):
        w1_bf = w_in[layer_idx].astype(jnp.bfloat16)
        w2_bf = w_out[layer_idx].astype(jnp.bfloat16)
        h_f32 = hidden.astype(jnp.float32)
        normed = rms_norm(h_f32).astype(jnp.bfloat16)
        pre_act = jnp.dot(normed, w1_bf, preferred_element_type=jnp.float32)
        act_bf = gelu_exact(pre_act).astype(jnp.bfloat16)
        hidden = (h_f32 + jnp.dot(act_bf, w2_bf, preferred_element_type=jnp.float32)).astype(jnp.bfloat16)
        saved_acts.append((w1_bf, w2_bf, h_f32, normed, pre_act, act_bf))
    grad_h = (hidden.astype(jnp.float32) - rows_tgt.astype(jnp.float32)) * (2.0 / (BATCH * D))
    grads_in = [None] * LAYERS
    grads_out = [None] * LAYERS
    for layer_idx in reversed(range(LAYERS)):
        w1_bf, w2_bf, h_f32, normed, pre_act, act_bf = saved_acts[layer_idx]
        grad_bf = grad_h.astype(jnp.bfloat16)
        grads_out[layer_idx] = jnp.dot(act_bf.T, grad_bf, preferred_element_type=jnp.float32)
        d_pre = (jnp.dot(grad_bf, w2_bf.T, preferred_element_type=jnp.float32) * gelu_slope(pre_act)).astype(jnp.bfloat16)
        grads_in[layer_idx] = jnp.dot(normed.T, d_pre, preferred_element_type=jnp.float32)
        if layer_idx > 0:
            grad_h = grad_h + rms_back(h_f32, jnp.dot(d_pre, w1_bf.T, preferred_element_type=jnp.float32))
    return jnp.stack(grads_in), jnp.stack(grads_out)


def all_grads(w_in, w_out, rows_in, rows_tgt):
    dev_count = ROWS * COLS

    def one_device(operands):
        return device_grads(operands[0], operands[1], operands[2], operands[3])

    grads_in, grads_out = lax.map(one_device, (
        w_in.reshape((dev_count,) + w_in.shape[2:]),
        w_out.reshape((dev_count,) + w_out.shape[2:]),
        rows_in.reshape((dev_count,) + rows_in.shape[2:]),
        rows_tgt.reshape((dev_count,) + rows_tgt.shape[2:])))
    return grads_in.reshape(w_in.shape), grads_out.reshape(w_out.shape)


def neighbour_mix(params):
    wire_copy = params.astype(jnp.bfloat16)
    mix_sum = params + jnp.roll(wire_copy, 1, axis=1).astype(jnp.float32)
    mix_sum = mix_sum + jnp.roll(wire_copy, -1, axis=1).astype(jnp.float32)
    mix_sum = mix_sum + jnp.roll(wire_copy, 1, axis=0).astype(jnp.float32)
    mix_sum = mix_sum + jnp.roll(wire_copy, -1, axis=0).astype(jnp.float32)
    return mix_sum / 5.0


def reference(w_in, w_out, inputs, targets):
    def window_body(carry, window_idx):
        cur_in, cur_out = carry
        step_a = 2 * window_idx
        rows_a = lax.dynamic_index_in_dim(inputs, step_a, axis=2, keepdims=False)
        tgt_a = lax.dynamic_index_in_dim(targets, step_a, axis=2, keepdims=False)
        rows_b = lax.dynamic_index_in_dim(inputs, step_a + 1, axis=2, keepdims=False)
        tgt_b = lax.dynamic_index_in_dim(targets, step_a + 1, axis=2, keepdims=False)
        g_a_in, g_a_out = all_grads(cur_in, cur_out, rows_a, tgt_a)
        g_b_in, g_b_out = all_grads(cur_in - LEARN_RATE * g_a_in, cur_out - LEARN_RATE * g_a_out, rows_b, tgt_b)
        new_in = neighbour_mix(cur_in) - LEARN_RATE * (g_a_in + g_b_in)
        new_out = neighbour_mix(cur_out) - LEARN_RATE * (g_a_out + g_b_out)
        return (new_in, new_out), None

    final_pair = lax.scan(window_body, (w_in, w_out), jnp.arange(WINDOWS))[0]
    return final_pair[0], final_pair[1]
```

```python
import functools

import jax
import jax.numpy as jnp
from jax import lax
from jax.experimental import pallas as pl
from jax.experimental.pallas import tpu as pltpu
from jax.sharding import PartitionSpec as P


LR_SCALE = 0.8
EPS = 1e-6
INV_SQRT2 = 0.7071067811865476
INV_SQRT_2PI = 0.3989422804014327
F32 = jnp.float32
BF16 = jnp.bfloat16
CONTRACT_ROWS = (((0,), (0,)), ((), ()))
CONTRACT_LAST = (((1,), (1,)), ((), ()))
VMEM_LIMIT = 63 * 1024 * 1024
TILE = 512
SLAB = 256
FWD_BLOCK = 512
BWD_BLOCK = 256
CHUNKS = 4
ANY = pl.BlockSpec(memory_space=pl.ANY)


def params_of(axes=1, limit=VMEM_LIMIT):
    return pltpu.CompilerParams(dimension_semantics=("arbitrary",) * axes, vmem_limit_bytes=limit)


def inv_rms_of(rows):
    return lax.rsqrt(jnp.mean(rows * rows, axis=-1, keepdims=True) + EPS)


def slabs(count, body):
    lax.fori_loop(0, count, lambda i, c: (body(pl.ds(pl.multiple_of(i * SLAB, SLAB), SLAB)), c)[1], 0)


def fwd_kernel(last, scale, t, *refs):
    if last:
        h_ref, w1_ref, w2_ref, tgt_hbm, act_ref, slope_ref, ut_hbm, hout_hbm, g_hbm, u_s, ut_s, acc, h_s, g_s, tgt_s, sems = refs
    else:
        h_ref, w1_ref, w2_ref, act_ref, slope_ref, ut_hbm, hout_hbm, u_s, ut_s, acc, h_s, sems = refs
    step = pl.program_id(0)
    rows_total = h_ref.shape[0]
    ut_copy = pltpu.make_async_copy(ut_s, ut_hbm, sems.at[0])
    hout_copy = pltpu.make_async_copy(h_s, hout_hbm, sems.at[1])
    if last:
        tgt_copy = pltpu.make_async_copy(tgt_hbm.at[0, 0, t], tgt_s, sems.at[2])
        g_copy = pltpu.make_async_copy(g_s, g_hbm, sems.at[3])

    @pl.when(step == 0)
    def _():
        if last:
            tgt_copy.start()

        for i in range(rows_total // SLAB):
            rows = pl.ds(i * SLAB, SLAB)
            h = h_ref[rows, :].astype(F32)
            u = h * inv_rms_of(h)
            u_s[rows, :] = u.astype(BF16)
            ut_s[:, rows] = u.T.astype(BF16)
            acc[rows, :] = jnp.zeros_like(h)
        ut_copy.start()

    for i in range(rows_total // TILE):
        rows = pl.ds(i * TILE, TILE)
        z = jnp.dot(u_s[rows, :], w1_ref[...], preferred_element_type=F32)
        half = 0.5 * (1.0 + lax.erf(z * INV_SQRT2))
        act = (z * half).astype(BF16)
        act_ref[rows, :] = act
        slope_ref[rows, :] = half + z * jnp.exp(-0.5 * z * z) * INV_SQRT_2PI
        acc[rows, :] += jnp.dot(act, w2_ref[...], preferred_element_type=F32)

    @pl.when(step == pl.num_programs(0) - 1)
    def _():
        if last:
            tgt_copy.wait()

        def finish(rows):
            h = (h_ref[rows, :].astype(F32) + acc[rows, :]).astype(BF16)
            h_s[rows, :] = h
            if last:
                g_s[rows, :] = ((h.astype(F32) - tgt_s[rows, :].astype(F32)) * scale).astype(BF16)

        slabs(rows_total // SLAB, finish)
        hout_copy.start()
        if last:
            g_copy.start()
        ut_copy.wait()
        hout_copy.wait()
        if last:
            g_copy.wait()


def forward(h, h_spec, w1, w2, target=None, scale=None, t=None):
    depth, ff = w1.shape
    rows = h.shape[-2]
    last = target is not None
    block = FWD_BLOCK
    in_specs = [
        h_spec or pl.BlockSpec((rows, depth), lambda j: (0, 0), pipeline_mode=pl.Buffered(1)),
        pl.BlockSpec((depth, block), lambda j: (0, j)),
        pl.BlockSpec((block, depth), lambda j: (j, 0)),
    ]
    out_shape = [
        jax.ShapeDtypeStruct((rows, ff), BF16),
        jax.ShapeDtypeStruct((rows, ff), F32),
        jax.ShapeDtypeStruct((depth, rows), BF16),
        jax.ShapeDtypeStruct((rows, depth), BF16),
    ]
    out_specs = [
        pl.BlockSpec((rows, block), lambda j: (0, j)),
        pl.BlockSpec((rows, block), lambda j: (0, j)),
        ANY,
        ANY,
    ]
    scratch = [
        pltpu.VMEM((rows, depth), BF16),
        pltpu.VMEM((depth, rows), BF16),
        pltpu.VMEM((rows, depth), F32),
        pltpu.VMEM((rows, depth), BF16),
    ]
    args = [h, w1, w2]
    if last:
        args.append(target)
        in_specs.append(ANY)
        out_shape.append(jax.ShapeDtypeStruct((rows, depth), BF16))
        out_specs.append(ANY)
        scratch += [pltpu.VMEM((rows, depth), BF16), pltpu.VMEM((rows, depth), BF16)]
    scratch.append(pltpu.SemaphoreType.DMA((4,)))
    return pl.pallas_call(
        functools.partial(fwd_kernel, last, scale, t),
        grid=(ff // block,),
        in_specs=in_specs, out_specs=out_specs, out_shape=out_shape, scratch_shapes=scratch,
        compiler_params=params_of(),
        cost_estimate=pl.CostEstimate(flops=4 * rows * depth * ff, bytes_accessed=rows * ff * 6 + depth * ff * 4,
                                      transcendentals=2 * rows * ff),
    )(*args)


def bwd_kernel(deep, second, scale, rate, t, *refs):
    refs = list(refs)
    g_ref, ut_ref, act_ref, slope_ref, w2_ref = refs[:5]
    rest = refs[5:]
    if deep:
        w1_ref, h_hbm, hl_hbm, tgt_hbm = rest[:4]
        rest = rest[4:]
    old1_ref, old2_ref = rest[:2]
    rest = rest[2:]
    d1_ref, d2_ref = rest[:2]
    rest = rest[2:]
    if not second:
        q1_ref, q2_ref = rest[:2]
        rest = rest[2:]
    if deep:
        gout_hbm = rest[0]
        rest = rest[1:]
    s_s = rest[0]
    if deep:
        acc, h_s, hl_s, tgt_s, gout_s, sems = rest[1:]
    step = pl.program_id(0)
    rows_total = g_ref.shape[0]
    if deep:
        loads = [pltpu.make_async_copy(src, dst, sems.at[i])
                 for i, (src, dst) in enumerate(((h_hbm, h_s), (hl_hbm, hl_s), (tgt_hbm.at[0, 0, t], tgt_s)))]
        gout_copy = pltpu.make_async_copy(gout_s, gout_hbm, sems.at[3])

        @pl.when(step == 0)
        def _():
            for load in loads:
                load.start()
            slabs(rows_total // SLAB, lambda rows: acc.__setitem__((rows, slice(None)), jnp.zeros((SLAB, acc.shape[1]), F32)))

    for i in range(rows_total // TILE):
        rows = pl.ds(i * TILE, TILE)
        back = lax.dot_general(g_ref[rows, :], w2_ref[...], CONTRACT_LAST, preferred_element_type=F32)
        s_s[rows, :] = (back * slope_ref[rows, :]).astype(BF16)

    d2 = lax.dot_general(act_ref[...], g_ref[...], CONTRACT_ROWS, preferred_element_type=F32)
    d1 = jnp.dot(ut_ref[...], s_s[...], preferred_element_type=F32)
    if second:
        d2_ref[...] = old2_ref[...] + d2
        d1_ref[...] = old1_ref[...] + d1
    else:
        d2_ref[...] = d2
        d1_ref[...] = d1
        q2_ref[...] = (old2_ref[...] - rate * d2).astype(BF16)
        q1_ref[...] = (old1_ref[...] - rate * d1).astype(BF16)
    if deep:
        for i in range(rows_total // TILE):
            rows = pl.ds(i * TILE, TILE)
            acc[rows, :] += lax.dot_general(s_s[rows, :], w1_ref[...], CONTRACT_LAST, preferred_element_type=F32)

        @pl.when(step == pl.num_programs(0) - 1)
        def _():
            for load in loads:
                load.wait()

            def finish(rows):
                h = h_s[rows, :].astype(F32)
                grad = acc[rows, :]
                inv_rms = inv_rms_of(h)
                row_dot = jnp.mean(h * grad, axis=-1, keepdims=True)
                e = (hl_s[rows, :].astype(F32) - tgt_s[rows, :].astype(F32)) * scale
                e = e + (inv_rms * grad - h * (inv_rms * inv_rms * inv_rms) * row_dot)
                gout_s[rows, :] = e.astype(BF16)

            slabs(rows_total // SLAB, finish)
            gout_copy.start()
            gout_copy.wait()


def backward(g, ut, act, slope, w1, w2, old1, old2, second, rate, layer, deep=None, scale=None, t=None):
    rows, ff = act.shape
    depth = g.shape[1]
    is_deep = deep is not None
    block = BWD_BLOCK
    if second:
        old1_spec = pl.BlockSpec((depth, block), lambda j: (0, j))
        old2_spec = pl.BlockSpec((block, depth), lambda j: (j, 0))
    else:
        old1_spec = pl.BlockSpec((None, None, None, depth, block), lambda j: (0, 0, layer, 0, j))
        old2_spec = pl.BlockSpec((None, None, None, block, depth), lambda j: (0, 0, layer, j, 0))
    once = pl.Buffered(1)
    args = [g, ut, act, slope, w2]
    in_specs = [
        pl.BlockSpec((rows, depth), lambda j: (0, 0), pipeline_mode=once),
        pl.BlockSpec((depth, rows), lambda j: (0, 0), pipeline_mode=once),
        pl.BlockSpec((rows, block), lambda j: (0, j)),
        pl.BlockSpec((rows, block), lambda j: (0, j)),
        pl.BlockSpec((block, depth), lambda j: (j, 0)),
    ]
    if is_deep:
        args += [w1, *deep]
        in_specs += [pl.BlockSpec((depth, block), lambda j: (0, j)), ANY, ANY, ANY]
    args += [old1, old2]
    in_specs += [old1_spec, old2_spec]
    out_shape = [jax.ShapeDtypeStruct((depth, ff), F32), jax.ShapeDtypeStruct((ff, depth), F32)]
    out_specs = [pl.BlockSpec((depth, block), lambda j: (0, j)), pl.BlockSpec((block, depth), lambda j: (j, 0))]
    if not second:
        out_shape += [jax.ShapeDtypeStruct((depth, ff), BF16), jax.ShapeDtypeStruct((ff, depth), BF16)]
        out_specs += out_specs[:2]
    scratch = [pltpu.VMEM((rows, block), BF16)]
    if is_deep:
        out_shape.append(jax.ShapeDtypeStruct((rows, depth), BF16))
        out_specs.append(ANY)
        scratch += [pltpu.VMEM((rows, depth), F32)] + [pltpu.VMEM((rows, depth), BF16)] * 4 + [pltpu.SemaphoreType.DMA((4,))]
    return pl.pallas_call(
        functools.partial(bwd_kernel, is_deep, second, scale, rate, t),
        grid=(ff // block,),
        in_specs=in_specs, out_specs=out_specs, out_shape=out_shape, scratch_shapes=scratch,
        compiler_params=params_of(),
        cost_estimate=pl.CostEstimate(flops=(8 if is_deep else 6) * rows * depth * ff,
                                      bytes_accessed=rows * ff * 6 + depth * ff * 24, transcendentals=0),
    )(*args)


def chunk_specs(shape, layer, part, steps):
    rows, cols = shape
    band = rows // CHUNKS // steps
    first = part * steps
    return (pl.BlockSpec((None, None, None, band, cols), lambda j: (0, 0, layer, first + j, 0)),
            pl.BlockSpec((band, cols), lambda j: (first + j, 0)),
            pl.BlockSpec((band, cols), lambda j: (j, 0)))


def cast_kernel(has_prev, p_ref, *refs):
    whole_ref, wire_ref = refs[1:] if has_prev else refs
    value = p_ref[...].astype(BF16)
    whole_ref[...] = value
    wire_ref[...] = value


def cast_chunk(p, layer, part, prev):
    shape = p.shape[-2:]
    steps = 2
    param_spec, layer_spec, wire_spec = chunk_specs(shape, layer, part, steps)
    return pl.pallas_call(
        functools.partial(cast_kernel, prev is not None),
        grid=(steps,),
        in_specs=[param_spec] + ([ANY] if prev is not None else []),
        out_specs=[layer_spec, wire_spec],
        out_shape=[jax.ShapeDtypeStruct(shape, BF16), jax.ShapeDtypeStruct((shape[0] // CHUNKS, shape[1]), BF16)],
        input_output_aliases={1: 0} if prev is not None else {},
        compiler_params=params_of(),
        cost_estimate=pl.CostEstimate(flops=10 ** 9, bytes_accessed=8 * shape[0] * shape[1] // CHUNKS, transcendentals=0),
    )(*([p] + ([prev] if prev is not None else [])))


def mix_kernel(rate, n_prev, final, par_ref, p_ref, grad_ref, col_ref, near_ref, far_ref, *refs):
    refs = refs[n_prev:]
    near = near_ref[...].astype(F32)
    far = far_ref[...].astype(F32)
    even = par_ref[0] == 0
    col = col_ref[...].astype(F32)
    mix = p_ref[...] + col + col
    mix = mix + jnp.where(even, far, near)
    mix = mix + jnp.where(even, near, far)
    new = mix / 5.0 - rate * grad_ref[...]
    refs[0][...] = new
    if not final:
        value = new.astype(BF16)
        refs[1][...] = value
        refs[2][...] = value


def mix_chunk(par, p, grad, col, near, far, layer, part, rate, prev_param, prev_layer, final):
    shape = p.shape[-2:]
    steps = 4
    param_spec, layer_spec, wire_spec = chunk_specs(shape, layer, part, steps)
    args = [par, p, grad, col, near, far]
    in_specs = [pl.BlockSpec(memory_space=pltpu.SMEM), param_spec, layer_spec, layer_spec, wire_spec, wire_spec]
    aliases = {}
    out_shape = [jax.ShapeDtypeStruct(p.shape, F32)]
    out_specs = [param_spec]
    if not final:
        out_shape += [jax.ShapeDtypeStruct(shape, BF16), jax.ShapeDtypeStruct((shape[0] // CHUNKS, shape[1]), BF16)]
        out_specs += [layer_spec, wire_spec]
    n_prev = 0
    for prev, out_idx in ((prev_param, 0), (None if final else prev_layer, 1)):
        if prev is not None:
            aliases[len(args)] = out_idx
            args.append(prev)
            in_specs.append(ANY)
            n_prev += 1
    return pl.pallas_call(
        functools.partial(mix_kernel, rate, n_prev, final),
        grid=(steps,),
        in_specs=in_specs, out_specs=out_specs, out_shape=out_shape,
        input_output_aliases=aliases,
        compiler_params=params_of(),
        cost_estimate=pl.CostEstimate(flops=10 ** 9, bytes_accessed=20 * shape[0] * shape[1] // CHUNKS, transcendentals=0),
    )(*args)


def solution(mesh):
    row_size = mesh.shape["row"]
    col_size = mesh.shape["col"]
    layers, windows = 2, 2
    near_pairs = [(i, i ^ 1) for i in range(row_size)]
    far_pairs = [(i, i ^ 2) for i in range(row_size)]
    col_pairs = [(i, (i + 1) % col_size) for i in range(col_size)]
    total = 2 * layers * CHUNKS

    def locate(i):
        return i // (2 * CHUNKS), (i // CHUNKS) % 2, i % CHUNKS

    def device_program(w_in, w_out, inputs, targets):
        batch, depth = inputs.shape[-2:]
        scale = 2.0 / (batch * depth)
        rate = LR_SCALE / layers
        par = (lax.axis_index("row") % 2).astype(jnp.int32).reshape(1)
        row_spec = lambda t: pl.BlockSpec((None, None, None, batch, depth), lambda j: (0, 0, t, 0, 0), pipeline_mode=pl.Buffered(1))

        def send(i, wire, weights):
            near = lax.ppermute(wire, "row", near_pairs)
            far = lax.ppermute(near, "row", far_pairs)
            cols = None
            if i % CHUNKS == CHUNKS - 1:
                layer, kind, _ = locate(i)
                cols = lax.ppermute(weights[layer][kind], "col", col_pairs)
            return near, far, cols

        def fwd(layer, h, weights, t):
            spec = row_spec(t) if layer == 0 else None
            if layer == layers - 1:
                return forward(h, spec, *weights[layer], target=targets, scale=scale, t=t)
            return forward(h, spec, *weights[layer])

        def grads(step, weights, t, olds, head=None):
            outs = head or run_forward(weights, t)
            g = outs[-1][4]
            found = [None] * layers
            for layer in reversed(range(layers)):
                act, slope, ut = outs[layer][:3]
                deep = (outs[layer - 1][3], outs[layer][3], targets) if layer else None
                res = backward(g, ut, act, slope,
                             *weights[layer], *olds[layer], step == 1, rate, layer, deep, scale, t)
                if layer:
                    g = res[-1]
                found[layer] = res
            return found

        def run_forward(weights, t):
            outs, h = [], inputs
            for layer in range(layers):
                outs.append(fwd(layer, h, weights, t))
                h = outs[-1][3]
            return outs

        params = [w_in, w_out]
        weights = [[None, None] for _ in range(layers)]
        moved = []
        for i in range(total):
            layer, kind, part = locate(i)
            weights[layer][kind], wire = cast_chunk(params[kind], layer, part, weights[layer][kind])
            moved.append(send(i, wire, weights))
        head = run_forward(weights, 0)
        for window in range(windows):
            final = window == windows - 1
            step_a = 2 * window
            first = grads(0, weights, step_a, [params] * layers, head)
            second = grads(1, [r[2:4] for r in first], step_a + 1, [r[:2] for r in first])
            new_params = [None, None]
            new_weights = [[None, None] for _ in range(layers)]
            new_moved, head = [], []
            for i in range(total):
                layer, kind, part = locate(i)
                near, far, _ = moved[i]
                cols = moved[i - i % CHUNKS + CHUNKS - 1][2]
                res = mix_chunk(par, params[kind], second[layer][kind], cols, near, far,
                             layer, part, rate, new_params[kind], new_weights[layer][kind], final)
                new_params[kind] = res[0]
                if not final:
                    new_weights[layer][kind] = res[1]
                    new_moved.append(send(i, res[2], new_weights))
                    if i % (2 * CHUNKS) == 2 * CHUNKS - 1:
                        h = inputs if layer == 0 else head[-1][3]
                        head.append(fwd(layer, h, new_weights, step_a + 2))
            params, weights, moved = new_params, new_weights, new_moved
        return params[0], params[1]

    block_spec = P("row", "col")
    return jax.shard_map(device_program, mesh=mesh, in_specs=(block_spec,) * 4, out_specs=(block_spec,) * 2, check_vma=False)
```

```python
import functools

import jax
import jax.numpy as jnp
from jax import lax
from jax.experimental import pallas as pl
from jax.experimental.pallas import tpu as pltpu
from jax.sharding import PartitionSpec as P


LR_SCALE = 0.8
EPS = 1e-6
INV_SQRT2 = 0.7071067811865476
INV_SQRT_2PI = 0.3989422804014327
F32 = jnp.float32
BF16 = jnp.bfloat16
CONTRACT_ROWS = (((0,), (0,)), ((), ()))
CONTRACT_LAST = (((1,), (1,)), ((), ()))
VMEM_LIMIT = 63 * 1024 * 1024
TILE = 512
SLAB = 256
FWD_BLOCK = 512
BWD_BLOCK = 256
HID_TILE = 256
PARTS = 2
CHUNKS = 4
ANY = pl.BlockSpec(memory_space=pl.ANY)


def params_of(axes=1, limit=VMEM_LIMIT):
    return pltpu.CompilerParams(dimension_semantics=("arbitrary",) * axes, vmem_limit_bytes=limit)


def inv_rms_of(rows):
    return lax.rsqrt(jnp.mean(rows * rows, axis=-1, keepdims=True) + EPS)


def slabs(count, body):
    lax.fori_loop(0, count, lambda i, c: (body(pl.ds(pl.multiple_of(i * SLAB, SLAB), SLAB)), c)[1], 0)


def act_kernel(h_ref, w1_ref, act_ref, slope_ref, ut_hbm, u_s, ut_s, sem):
    step = pl.program_id(0)
    rows_total = h_ref.shape[0]
    ut_copy = pltpu.make_async_copy(ut_s, ut_hbm, sem)

    @pl.when(step == 0)
    def _():
        def normalize(rows):
            h = h_ref[rows, :].astype(F32)
            u = h * inv_rms_of(h)
            u_s[rows, :] = u.astype(BF16)
            ut_s[:, rows] = u.T.astype(BF16)

        slabs(rows_total // SLAB, normalize)
        ut_copy.start()

    for i in range(rows_total // TILE):
        rows = pl.ds(i * TILE, TILE)
        z = jnp.dot(u_s[rows, :], w1_ref[...], preferred_element_type=F32)
        half = 0.5 * (1.0 + lax.erf(z * INV_SQRT2))
        act_ref[rows, :] = (z * half).astype(BF16)
        slope_ref[rows, :] = half + z * jnp.exp(-0.5 * z * z) * INV_SQRT_2PI

    @pl.when(step == pl.num_programs(0) - 1)
    def _():
        ut_copy.wait()


def activate(h, t, w1):
    depth, ff = w1.shape
    rows = h.shape[-2]
    block = FWD_BLOCK
    once = pl.Buffered(1)
    if t is None:
        h_spec = pl.BlockSpec((rows, depth), lambda j: (0, 0), pipeline_mode=once)
    else:
        h_spec = pl.BlockSpec((None, None, None, rows, depth), lambda j: (0, 0, t, 0, 0), pipeline_mode=once)
    return pl.pallas_call(
        act_kernel,
        grid=(ff // block,),
        in_specs=[h_spec, pl.BlockSpec((depth, block), lambda j: (0, j))],
        out_specs=[pl.BlockSpec((rows, block), lambda j: (0, j)), pl.BlockSpec((rows, block), lambda j: (0, j)), ANY],
        out_shape=[jax.ShapeDtypeStruct((rows, ff), BF16), jax.ShapeDtypeStruct((rows, ff), F32),
                   jax.ShapeDtypeStruct((depth, rows), BF16)],
        scratch_shapes=[pltpu.VMEM((rows, depth), BF16), pltpu.VMEM((depth, rows), BF16), pltpu.SemaphoreType.DMA],
        compiler_params=params_of(),
        cost_estimate=pl.CostEstimate(flops=2 * rows * depth * ff, bytes_accessed=rows * ff * 6 + depth * ff * 2,
                                      transcendentals=2 * rows * ff),
    )(h, w1)


def hidden_kernel(last, scale, act_ref, w2_ref, h_ref, *refs):
    add = jnp.dot(act_ref[...], w2_ref[...], preferred_element_type=F32)
    h = (h_ref[...].astype(F32) + add).astype(BF16)
    if last:
        tgt_ref, hout_ref, g_ref = refs
        g_ref[...] = ((h.astype(F32) - tgt_ref[...].astype(F32)) * scale).astype(BF16)
    else:
        hout_ref, = refs
    hout_ref[...] = h


def hidden(act, w2, h, t, target, target_t, scale):
    ff, depth = w2.shape
    rows = act.shape[0]
    tile = HID_TILE
    plain = pl.BlockSpec((tile, depth), lambda i: (i, 0))
    of_step = lambda t: pl.BlockSpec((None, None, None, tile, depth), lambda i: (0, 0, t, i, 0))
    last = target is not None
    n_out = 2 if last else 1
    return pl.pallas_call(
        functools.partial(hidden_kernel, last, scale),
        grid=(rows // tile,),
        in_specs=[pl.BlockSpec((tile, ff), lambda i: (i, 0)),
                  pl.BlockSpec((ff, depth), lambda i: (0, 0), pipeline_mode=pl.Buffered(1)),
                  plain if t is None else of_step(t)] + ([of_step(target_t)] if last else []),
        out_specs=[plain] * n_out,
        out_shape=[jax.ShapeDtypeStruct((rows, depth), BF16)] * n_out,
        compiler_params=params_of(),
        cost_estimate=pl.CostEstimate(flops=2 * rows * depth * ff, bytes_accessed=rows * ff * 2 + depth * ff * 2,
                                      transcendentals=0),
    )(act, w2, h, *([target] if last else []))


def bwd_kernel(deep, second, part, scale, rate, t, n_prev, *refs):
    refs = list(refs)

    def take(count):
        taken = refs[:count]
        del refs[:count]
        return taken

    g_ref, ut_ref, act_ref, slope_ref, w2_ref = take(5)
    closing = deep and part == PARTS - 1
    if deep:
        w1_ref, = take(1)
    if deep and part:
        acc_in_hbm, = take(1)
    if closing:
        h_hbm, hl_hbm, tgt_hbm = take(3)
    old1_ref, old2_ref = take(2)
    take(n_prev)
    d1_ref, d2_ref = take(2)
    if not second:
        q1_ref, q2_ref = take(2)
    if deep:
        out_hbm, = take(1)
    s_s, = take(1)
    if deep:
        acc, sems = take(2)
    if closing:
        h_s, hl_s, tgt_s, gout_s = take(4)
    step = pl.program_id(0)
    rows_total = g_ref.shape[0]
    if deep:
        @pl.when(step == 0)
        def _():
            if part:
                acc_load = pltpu.make_async_copy(acc_in_hbm, acc, sems.at[0])
                acc_load.start()
                acc_load.wait()
            else:
                def clear(rows):
                    acc[rows, :] = jnp.zeros((SLAB, acc.shape[1]), F32)

                slabs(rows_total // SLAB, clear)
    if closing:
        loads = [pltpu.make_async_copy(src, dst, sems.at[i + 1])
                 for i, (src, dst) in enumerate(((h_hbm, h_s), (hl_hbm, hl_s), (tgt_hbm.at[0, 0, t], tgt_s)))]

        @pl.when(step == 0)
        def _():
            for load in loads:
                load.start()

    for i in range(rows_total // TILE):
        rows = pl.ds(i * TILE, TILE)
        back = lax.dot_general(g_ref[rows, :], w2_ref[...], CONTRACT_LAST, preferred_element_type=F32)
        s_s[rows, :] = (back * slope_ref[rows, :]).astype(BF16)

    d2 = lax.dot_general(act_ref[...], g_ref[...], CONTRACT_ROWS, preferred_element_type=F32)
    d1 = jnp.dot(ut_ref[...], s_s[...], preferred_element_type=F32)
    if second:
        d2_ref[...] = old2_ref[...] + d2
        d1_ref[...] = old1_ref[...] + d1
    else:
        d2_ref[...] = d2
        d1_ref[...] = d1
        q2_ref[...] = (old2_ref[...] - rate * d2).astype(BF16)
        q1_ref[...] = (old1_ref[...] - rate * d1).astype(BF16)
    if deep:
        for i in range(rows_total // TILE):
            rows = pl.ds(i * TILE, TILE)
            acc[rows, :] += lax.dot_general(s_s[rows, :], w1_ref[...], CONTRACT_LAST, preferred_element_type=F32)

        @pl.when(step == pl.num_programs(0) - 1)
        def _():
            out_copy = pltpu.make_async_copy(gout_s if closing else acc, out_hbm, sems.at[0])
            if closing:
                for load in loads:
                    load.wait()

                def finish(rows):
                    h = h_s[rows, :].astype(F32)
                    grad = acc[rows, :]
                    inv_rms = inv_rms_of(h)
                    row_dot = jnp.mean(h * grad, axis=-1, keepdims=True)
                    e = (hl_s[rows, :].astype(F32) - tgt_s[rows, :].astype(F32)) * scale
                    e = e + (inv_rms * grad - h * (inv_rms * inv_rms * inv_rms) * row_dot)
                    gout_s[rows, :] = e.astype(BF16)

                slabs(rows_total // SLAB, finish)
            out_copy.start()
            out_copy.wait()


def backward(part, g, ut, act, slope, w1, w2, old1, old2, prev, second, rate, layer, deep, scale, t):
    rows, ff = act.shape
    depth = g.shape[1]
    is_deep = deep is not None
    closing = is_deep and part == PARTS - 1
    block = BWD_BLOCK
    steps = ff // block // PARTS
    first = part * steps
    in_cols = pl.BlockSpec((depth, block), lambda j: (0, first + j))
    out_rows = pl.BlockSpec((block, depth), lambda j: (first + j, 0))
    wide = pl.BlockSpec((rows, block), lambda j: (0, first + j))
    if second:
        old_specs = [in_cols, out_rows]
    else:
        old_specs = [pl.BlockSpec((None, None, None, depth, block), lambda j: (0, 0, layer, 0, first + j)),
                     pl.BlockSpec((None, None, None, block, depth), lambda j: (0, 0, layer, first + j, 0))]
    once = pl.Buffered(1)
    args = [g, ut, act, slope, w2]
    in_specs = [pl.BlockSpec((rows, depth), lambda j: (0, 0), pipeline_mode=once),
                pl.BlockSpec((depth, rows), lambda j: (0, 0), pipeline_mode=once), wide, wide, out_rows]
    n_grads = 2 if second else 4
    if is_deep:
        args.append(w1)
        in_specs.append(in_cols)
    if is_deep and part:
        args.append(prev[-1])
        in_specs.append(ANY)
    if closing:
        args += list(deep)
        in_specs += [ANY] * 3
    args += [old1, old2]
    in_specs += old_specs
    aliases, n_prev = {}, 0
    if part:
        n_prev = n_grads
        for i in range(n_grads):
            aliases[len(args)] = i
            args.append(prev[i])
            in_specs.append(ANY)
    out_shape = [jax.ShapeDtypeStruct((depth, ff), F32), jax.ShapeDtypeStruct((ff, depth), F32)]
    out_specs = [in_cols, out_rows]
    if not second:
        out_shape += [jax.ShapeDtypeStruct((depth, ff), BF16), jax.ShapeDtypeStruct((ff, depth), BF16)]
        out_specs += [in_cols, out_rows]
    scratch = [pltpu.VMEM((rows, block), BF16)]
    if is_deep:
        out_shape.append(jax.ShapeDtypeStruct((rows, depth), BF16 if closing else F32))
        out_specs.append(ANY)
        scratch += [pltpu.VMEM((rows, depth), F32), pltpu.SemaphoreType.DMA((4,))]
    if closing:
        scratch += [pltpu.VMEM((rows, depth), BF16)] * 4
    return pl.pallas_call(
        functools.partial(bwd_kernel, is_deep, second, part, scale, rate, t, n_prev),
        grid=(steps,),
        in_specs=in_specs, out_specs=out_specs, out_shape=out_shape, scratch_shapes=scratch,
        input_output_aliases=aliases,
        compiler_params=params_of(),
        cost_estimate=pl.CostEstimate(flops=(8 if is_deep else 6) * rows * depth * ff // PARTS,
                                      bytes_accessed=(rows * ff * 6 + depth * ff * 24) // PARTS, transcendentals=0),
    )(*args)


def chunk_specs(shape, layer, part, steps):
    rows, cols = shape
    band = rows // CHUNKS // steps
    first = part * steps
    return (pl.BlockSpec((None, None, None, band, cols), lambda j: (0, 0, layer, first + j, 0)),
            pl.BlockSpec((band, cols), lambda j: (first + j, 0)),
            pl.BlockSpec((band, cols), lambda j: (j, 0)))


def cast_kernel(has_prev, p_ref, *refs):
    whole_ref, wire_ref = refs[1:] if has_prev else refs
    value = p_ref[...].astype(BF16)
    whole_ref[...] = value
    wire_ref[...] = value


def cast_chunk(p, layer, part, prev):
    shape = p.shape[-2:]
    steps = 2
    param_spec, layer_spec, wire_spec = chunk_specs(shape, layer, part, steps)
    return pl.pallas_call(
        functools.partial(cast_kernel, prev is not None),
        grid=(steps,),
        in_specs=[param_spec] + ([ANY] if prev is not None else []),
        out_specs=[layer_spec, wire_spec],
        out_shape=[jax.ShapeDtypeStruct(shape, BF16), jax.ShapeDtypeStruct((shape[0] // CHUNKS, shape[1]), BF16)],
        input_output_aliases={1: 0} if prev is not None else {},
        compiler_params=params_of(),
        cost_estimate=pl.CostEstimate(flops=10 ** 9, bytes_accessed=8 * shape[0] * shape[1] // CHUNKS, transcendentals=0),
    )(*([p] + ([prev] if prev is not None else [])))


def mix_kernel(rate, n_prev, final, par_ref, p_ref, grad_ref, col_ref, near_ref, far_ref, *refs):
    refs = refs[n_prev:]
    near = near_ref[...].astype(F32)
    far = far_ref[...].astype(F32)
    even = par_ref[0] == 0
    col = col_ref[...].astype(F32)
    mix = p_ref[...] + col + col
    mix = mix + jnp.where(even, far, near)
    mix = mix + jnp.where(even, near, far)
    new = mix / 5.0 - rate * grad_ref[...]
    refs[0][...] = new
    if not final:
        value = new.astype(BF16)
        refs[1][...] = value
        refs[2][...] = value


def mix_chunk(par, p, grad, col, near, far, layer, part, rate, prev_param, prev_layer, final):
    shape = p.shape[-2:]
    steps = 8
    param_spec, layer_spec, wire_spec = chunk_specs(shape, layer, part, steps)
    args = [par, p, grad, col, near, far]
    in_specs = [pl.BlockSpec(memory_space=pltpu.SMEM), param_spec, layer_spec, layer_spec, wire_spec, wire_spec]
    aliases = {}
    out_shape = [jax.ShapeDtypeStruct(p.shape, F32)]
    out_specs = [param_spec]
    if not final:
        out_shape += [jax.ShapeDtypeStruct(shape, BF16), jax.ShapeDtypeStruct((shape[0] // CHUNKS, shape[1]), BF16)]
        out_specs += [layer_spec, wire_spec]
    n_prev = 0
    for prev, out_idx in ((prev_param, 0), (None if final else prev_layer, 1)):
        if prev is not None:
            aliases[len(args)] = out_idx
            args.append(prev)
            in_specs.append(ANY)
            n_prev += 1
    return pl.pallas_call(
        functools.partial(mix_kernel, rate, n_prev, final),
        grid=(steps,),
        in_specs=in_specs, out_specs=out_specs, out_shape=out_shape,
        input_output_aliases=aliases,
        compiler_params=params_of(),
        cost_estimate=pl.CostEstimate(flops=10 ** 9, bytes_accessed=20 * shape[0] * shape[1] // CHUNKS, transcendentals=0),
    )(*args)


def solution(mesh):
    row_size = mesh.shape["row"]
    col_size = mesh.shape["col"]
    layers, windows = 2, 2
    near_pairs = [(i, i ^ 1) for i in range(row_size)]
    far_pairs = [(i, i ^ 2) for i in range(row_size)]
    col_pairs = [(i, (i + 1) % col_size) for i in range(col_size)]
    total = 2 * layers * CHUNKS

    def locate(i):
        return i // (2 * CHUNKS), (i // CHUNKS) % 2, i % CHUNKS

    def device_program(w_in, w_out, inputs, targets):
        batch, depth = inputs.shape[-2:]
        scale = 2.0 / (batch * depth)
        rate = LR_SCALE / layers
        par = (lax.axis_index("row") % 2).astype(jnp.int32).reshape(1)

        def send(i, wire, weights):
            near = lax.ppermute(wire, "row", near_pairs)
            far = lax.ppermute(near, "row", far_pairs)
            cols = None
            if i % CHUNKS == CHUNKS - 1:
                layer, kind, _ = locate(i)
                cols = lax.ppermute(weights[layer][kind], "col", col_pairs)
            return near, far, cols

        def fwd(layer, h, weights, t):
            w1, w2 = weights[layer]
            at = t if layer == 0 else None
            act, slope, ut = activate(h, at, w1)
            outs = hidden(act, w2, h, at, targets if layer == layers - 1 else None, t, scale)
            return (act, slope, ut, *outs)

        def run_forward(weights, t):
            outs, h = [], inputs
            for layer in range(layers):
                outs.append(fwd(layer, h, weights, t))
                h = outs[-1][3]
            return outs

        def grads(step, outs, weights, t, olds):
            g = outs[-1][4]
            found = [None] * layers
            for layer in reversed(range(layers)):
                act, slope, ut = outs[layer][:3]
                deep = (outs[layer - 1][3], outs[layer][3], targets) if layer else None
                res = None
                for part in range(PARTS):
                    res = backward(part, g, ut, act, slope,
                                 *weights[layer], *olds[layer], res, step == 1, rate, layer, deep, scale, t)
                if layer:
                    g = res[-1]
                found[layer] = res
            return found

        params = [w_in, w_out]
        weights = [[None, None] for _ in range(layers)]
        moved = []
        for i in range(total):
            layer, kind, part = locate(i)
            weights[layer][kind], wire = cast_chunk(params[kind], layer, part, weights[layer][kind])
            moved.append(send(i, wire, weights))
        head = run_forward(weights, 0)
        for window in range(windows):
            final = window == windows - 1
            step_a = 2 * window
            first = grads(0, head, weights, step_a, [params] * layers)
            moved_on = [r[2:4] for r in first]
            middle = run_forward(moved_on, step_a + 1)
            second = grads(1, middle, moved_on, step_a + 1, [r[:2] for r in first])
            new_params = [None, None]
            new_weights = [[None, None] for _ in range(layers)]
            new_moved, head = [], []
            for i in range(total):
                layer, kind, part = locate(i)
                near, far, _ = moved[i]
                cols = moved[i - i % CHUNKS + CHUNKS - 1][2]
                res = mix_chunk(par, params[kind], second[layer][kind], cols, near, far,
                             layer, part, rate, new_params[kind], new_weights[layer][kind], final)
                new_params[kind] = res[0]
                if not final:
                    new_weights[layer][kind] = res[1]
                    new_moved.append(send(i, res[2], new_weights))
                    if i % (2 * CHUNKS) == 2 * CHUNKS - 1:
                        h = inputs if layer == 0 else head[-1][3]
                        head.append(fwd(layer, h, new_weights, step_a + 2))
            params, weights, moved = new_params, new_weights, new_moved
        return params[0], params[1]

    block_spec = P("row", "col")
    return jax.shard_map(device_program, mesh=mesh, in_specs=(block_spec,) * 4, out_specs=(block_spec,) * 2, check_vma=False)
```

```python
import functools

import jax
import jax.numpy as jnp
from jax import lax
from jax.experimental import pallas as pl
from jax.experimental.pallas import tpu as pltpu
from jax.sharding import PartitionSpec as P


LR_SCALE = 0.8
EPS = 1e-6
INV_SQRT2 = 0.7071067811865476
INV_SQRT_2PI = 0.3989422804014327
F32 = jnp.float32
BF16 = jnp.bfloat16
CONTRACT_ROWS = (((0,), (0,)), ((), ()))
CONTRACT_LAST = (((1,), (1,)), ((), ()))
VMEM_LIMIT = 63 * 1024 * 1024
TILE = 512
ACT_TILE = 128
SLAB = 256
FWD_BLOCK = 512
BWD_BLOCK = 256
HID_TILE = 256
PARTS = (1, 2)
CHUNKS = 4
ANY = pl.BlockSpec(memory_space=pl.ANY)


def params_of(axes=1, limit=VMEM_LIMIT):
    return pltpu.CompilerParams(dimension_semantics=("arbitrary",) * axes, vmem_limit_bytes=limit)


def inv_rms_of(rows):
    return lax.rsqrt(jnp.mean(rows * rows, axis=-1, keepdims=True) + EPS)


def slabs(count, body):
    lax.fori_loop(0, count, lambda i, c: (body(pl.ds(pl.multiple_of(i * SLAB, SLAB), SLAB)), c)[1], 0)


def act_kernel(h_ref, w1_ref, act_ref, slope_ref, ut_hbm, u_s, ut_s, z_s, sem):
    step = pl.program_id(0)
    rows_total = h_ref.shape[0]
    ut_copy = pltpu.make_async_copy(ut_s, ut_hbm, sem)

    @pl.when(step == 0)
    def _():
        def normalize(rows):
            h = h_ref[rows, :].astype(F32)
            u = h * inv_rms_of(h)
            u_s[rows, :] = u.astype(BF16)
            ut_s[:, rows] = u.T.astype(BF16)

        slabs(rows_total // SLAB, normalize)
        ut_copy.start()

    for i in range(rows_total // ACT_TILE):
        rows = pl.ds(i * ACT_TILE, ACT_TILE)
        z = z_s[rows, :]
        half = 0.5 * (1.0 + lax.erf(z * INV_SQRT2))
        act_ref[rows, :] = (z * half).astype(BF16)
        slope_ref[rows, :] = half + z * jnp.exp(-0.5 * z * z) * INV_SQRT_2PI
        z_s[rows, :] = jnp.dot(u_s[rows, :], w1_ref[...], preferred_element_type=F32)

    @pl.when(step == pl.num_programs(0) - 1)
    def _():
        ut_copy.wait()


def activate(h, t, w1):
    depth, ff = w1.shape
    rows = h.shape[-2]
    block = FWD_BLOCK
    once = pl.Buffered(1)
    if t is None:
        h_spec = pl.BlockSpec((rows, depth), lambda j: (0, 0), pipeline_mode=once)
    else:
        h_spec = pl.BlockSpec((None, None, None, rows, depth), lambda j: (0, 0, t, 0, 0), pipeline_mode=once)
    blocks = ff // block
    done_block = pl.BlockSpec((rows, block), lambda j: (0, jnp.maximum(j - 1, 0)))
    return pl.pallas_call(
        act_kernel,
        grid=(blocks + 1,),
        in_specs=[h_spec, pl.BlockSpec((depth, block), lambda j: (0, jnp.minimum(j, blocks - 1)))],
        out_specs=[done_block, done_block, ANY],
        out_shape=[jax.ShapeDtypeStruct((rows, ff), BF16), jax.ShapeDtypeStruct((rows, ff), F32),
                   jax.ShapeDtypeStruct((depth, rows), BF16)],
        scratch_shapes=[pltpu.VMEM((rows, depth), BF16), pltpu.VMEM((depth, rows), BF16), pltpu.VMEM((rows, block), F32),
                        pltpu.SemaphoreType.DMA],
        compiler_params=params_of(),
        cost_estimate=pl.CostEstimate(flops=2 * rows * depth * ff, bytes_accessed=rows * ff * 6 + depth * ff * 2,
                                      transcendentals=2 * rows * ff),
    )(h, w1)


def hidden_kernel(last, scale, act_ref, w2_ref, h_ref, *refs):
    add = jnp.dot(act_ref[...], w2_ref[...], preferred_element_type=F32)
    h = (h_ref[...].astype(F32) + add).astype(BF16)
    if last:
        tgt_ref, hout_ref, g_ref = refs
        g_ref[...] = ((h.astype(F32) - tgt_ref[...].astype(F32)) * scale).astype(BF16)
    else:
        hout_ref, = refs
    hout_ref[...] = h


def hidden(act, w2, h, t, target, target_t, scale):
    ff, depth = w2.shape
    rows = act.shape[0]
    tile = HID_TILE
    plain = pl.BlockSpec((tile, depth), lambda i: (i, 0))
    of_step = lambda t: pl.BlockSpec((None, None, None, tile, depth), lambda i: (0, 0, t, i, 0))
    last = target is not None
    n_out = 2 if last else 1
    return pl.pallas_call(
        functools.partial(hidden_kernel, last, scale),
        grid=(rows // tile,),
        in_specs=[pl.BlockSpec((tile, ff), lambda i: (i, 0)),
                  pl.BlockSpec((ff, depth), lambda i: (0, 0), pipeline_mode=pl.Buffered(1)),
                  plain if t is None else of_step(t)] + ([of_step(target_t)] if last else []),
        out_specs=[plain] * n_out,
        out_shape=[jax.ShapeDtypeStruct((rows, depth), BF16)] * n_out,
        compiler_params=params_of(),
        cost_estimate=pl.CostEstimate(flops=2 * rows * depth * ff, bytes_accessed=rows * ff * 2 + depth * ff * 2,
                                      transcendentals=0),
    )(act, w2, h, *([target] if last else []))


def bwd_kernel(deep, second, part, scale, rate, t, n_prev, *refs):
    refs = list(refs)

    def take(count):
        taken = refs[:count]
        del refs[:count]
        return taken

    g_ref, ut_ref, act_ref, slope_ref, w2_ref = take(5)
    closing = deep and part == PARTS[1] - 1
    if deep:
        w1_ref, = take(1)
    if deep and part:
        acc_in_hbm, = take(1)
    if closing:
        h_hbm, hl_hbm, tgt_hbm = take(3)
    old1_ref, old2_ref = take(2)
    take(n_prev)
    d1_ref, d2_ref = take(2)
    if not second:
        q1_ref, q2_ref = take(2)
    if deep:
        out_hbm, = take(1)
    s_s, = take(1)
    if deep:
        acc, sems = take(2)
    if closing:
        h_s, hl_s, tgt_s, gout_s = take(4)
    step = pl.program_id(0)
    rows_total = g_ref.shape[0]
    if deep:
        @pl.when(step == 0)
        def _():
            if part:
                acc_load = pltpu.make_async_copy(acc_in_hbm, acc, sems.at[0])
                acc_load.start()
                acc_load.wait()
            else:
                def clear(rows):
                    acc[rows, :] = jnp.zeros((SLAB, acc.shape[1]), F32)

                slabs(rows_total // SLAB, clear)
    if closing:
        loads = [pltpu.make_async_copy(src, dst, sems.at[i + 1])
                 for i, (src, dst) in enumerate(((h_hbm, h_s), (hl_hbm, hl_s), (tgt_hbm.at[0, 0, t], tgt_s)))]

        @pl.when(step == 0)
        def _():
            for load in loads:
                load.start()

    for i in range(rows_total // TILE):
        rows = pl.ds(i * TILE, TILE)
        back = lax.dot_general(g_ref[rows, :], w2_ref[...], CONTRACT_LAST, preferred_element_type=F32)
        s_s[rows, :] = (back * slope_ref[rows, :]).astype(BF16)

    d2 = lax.dot_general(act_ref[...], g_ref[...], CONTRACT_ROWS, preferred_element_type=F32)
    d1 = jnp.dot(ut_ref[...], s_s[...], preferred_element_type=F32)
    if second:
        d2_ref[...] = old2_ref[...] + d2
        d1_ref[...] = old1_ref[...] + d1
    else:
        d2_ref[...] = d2
        d1_ref[...] = d1
        q2_ref[...] = (old2_ref[...] - rate * d2).astype(BF16)
        q1_ref[...] = (old1_ref[...] - rate * d1).astype(BF16)
    if deep:
        for i in range(rows_total // TILE):
            rows = pl.ds(i * TILE, TILE)
            acc[rows, :] += lax.dot_general(s_s[rows, :], w1_ref[...], CONTRACT_LAST, preferred_element_type=F32)

        @pl.when(step == pl.num_programs(0) - 1)
        def _():
            out_copy = pltpu.make_async_copy(gout_s if closing else acc, out_hbm, sems.at[0])
            if closing:
                for load in loads:
                    load.wait()

                def finish(rows):
                    h = h_s[rows, :].astype(F32)
                    grad = acc[rows, :]
                    inv_rms = inv_rms_of(h)
                    row_dot = jnp.mean(h * grad, axis=-1, keepdims=True)
                    e = (hl_s[rows, :].astype(F32) - tgt_s[rows, :].astype(F32)) * scale
                    e = e + (inv_rms * grad - h * (inv_rms * inv_rms * inv_rms) * row_dot)
                    gout_s[rows, :] = e.astype(BF16)

                slabs(rows_total // SLAB, finish)
            out_copy.start()
            out_copy.wait()


def backward(part, g, ut, act, slope, w1, w2, old1, old2, prev, second, rate, layer, deep, scale, t):
    rows, ff = act.shape
    depth = g.shape[1]
    is_deep = deep is not None
    parts = PARTS[layer]
    closing = is_deep and part == parts - 1
    block = BWD_BLOCK
    steps = ff // block // parts
    first = part * steps
    in_cols = pl.BlockSpec((depth, block), lambda j: (0, first + j))
    out_rows = pl.BlockSpec((block, depth), lambda j: (first + j, 0))
    wide = pl.BlockSpec((rows, block), lambda j: (0, first + j))
    if second:
        old_specs = [in_cols, out_rows]
    else:
        old_specs = [pl.BlockSpec((None, None, None, depth, block), lambda j: (0, 0, layer, 0, first + j)),
                     pl.BlockSpec((None, None, None, block, depth), lambda j: (0, 0, layer, first + j, 0))]
    once = pl.Buffered(1)
    args = [g, ut, act, slope, w2]
    in_specs = [pl.BlockSpec((rows, depth), lambda j: (0, 0), pipeline_mode=once),
                pl.BlockSpec((depth, rows), lambda j: (0, 0), pipeline_mode=once), wide, wide, out_rows]
    n_grads = 2 if second else 4
    if is_deep:
        args.append(w1)
        in_specs.append(in_cols)
    if is_deep and part:
        args.append(prev[-1])
        in_specs.append(ANY)
    if closing:
        args += list(deep)
        in_specs += [ANY] * 3
    args += [old1, old2]
    in_specs += old_specs
    aliases, n_prev = {}, 0
    if part:
        n_prev = n_grads
        for i in range(n_grads):
            aliases[len(args)] = i
            args.append(prev[i])
            in_specs.append(ANY)
    out_shape = [jax.ShapeDtypeStruct((depth, ff), F32), jax.ShapeDtypeStruct((ff, depth), F32)]
    out_specs = [in_cols, out_rows]
    if not second:
        out_shape += [jax.ShapeDtypeStruct((depth, ff), BF16), jax.ShapeDtypeStruct((ff, depth), BF16)]
        out_specs += [in_cols, out_rows]
    scratch = [pltpu.VMEM((rows, block), BF16)]
    if is_deep:
        out_shape.append(jax.ShapeDtypeStruct((rows, depth), BF16 if closing else F32))
        out_specs.append(ANY)
        scratch += [pltpu.VMEM((rows, depth), F32), pltpu.SemaphoreType.DMA((4,))]
    if closing:
        scratch += [pltpu.VMEM((rows, depth), BF16)] * 4
    return pl.pallas_call(
        functools.partial(bwd_kernel, is_deep, second, part, scale, rate, t, n_prev),
        grid=(steps,),
        in_specs=in_specs, out_specs=out_specs, out_shape=out_shape, scratch_shapes=scratch,
        input_output_aliases=aliases,
        compiler_params=params_of(),
        cost_estimate=pl.CostEstimate(flops=(8 if is_deep else 6) * rows * depth * ff // parts,
                                      bytes_accessed=(rows * ff * 6 + depth * ff * 24) // parts, transcendentals=0),
    )(*args)


def chunk_specs(shape, layer, part, count, steps):
    rows, cols = shape
    band = rows // CHUNKS // steps
    first = part * steps

    def alone(m):
        return pl.BlockSpec((band, cols), lambda j: (jnp.clip(j - m * steps, 0, steps - 1), 0))

    return (pl.BlockSpec((None, None, None, band, cols), lambda j: (0, 0, layer, first + j, 0)),
            pl.BlockSpec((band, cols), lambda j: (first + j, 0)),
            [alone(m) for m in range(count)])


def in_turn(count, steps, body):
    if count == 1:
        return body(0)
    turn = pl.program_id(0) // steps
    for m in range(count):
        pl.when(turn == m)(functools.partial(body, m))


def cast_kernel(count, steps, n_prev, p_ref, *refs):
    whole_ref, *wire_refs = refs[n_prev:]
    value = p_ref[...].astype(BF16)
    whole_ref[...] = value

    def put(m):
        wire_refs[m][...] = value

    in_turn(count, steps, put)


def cast_chunks(p, layer, part, count, prev):
    shape = p.shape[-2:]
    steps = 2
    param_spec, layer_spec, wire_specs = chunk_specs(shape, layer, part, count, steps)
    args, in_specs = [p], [param_spec]
    if prev is not None:
        args.append(prev)
        in_specs.append(ANY)
    wire = jax.ShapeDtypeStruct((shape[0] // CHUNKS, shape[1]), BF16)
    return pl.pallas_call(
        functools.partial(cast_kernel, count, steps, len(args) - 1),
        grid=(count * steps,),
        in_specs=in_specs,
        out_specs=[layer_spec, *wire_specs],
        out_shape=[jax.ShapeDtypeStruct(shape, BF16)] + [wire] * count,
        input_output_aliases={1: 0} if prev is not None else {},
        compiler_params=params_of(),
        cost_estimate=pl.CostEstimate(flops=10 ** 9, bytes_accessed=8 * count * shape[0] * shape[1] // CHUNKS,
                                      transcendentals=0),
    )(*args)


def mix_kernel(rate, count, steps, n_prev, final, par_ref, p_ref, grad_ref, col_ref, *refs):
    near_refs, far_refs = refs[:count], refs[count:2 * count]
    outs = refs[2 * count + n_prev:]
    even = par_ref[0] == 0

    def mix_one(m):
        near = near_refs[m][...].astype(F32)
        far = far_refs[m][...].astype(F32)
        col = col_ref[...].astype(F32)
        mix = p_ref[...] + col + col
        mix = mix + jnp.where(even, far, near)
        mix = mix + jnp.where(even, near, far)
        new = mix / 5.0 - rate * grad_ref[...]
        outs[0][...] = new
        if not final:
            value = new.astype(BF16)
            outs[1][...] = value
            outs[2 + m][...] = value

    in_turn(count, steps, mix_one)


def mix_chunks(par, p, grad, col, nears, fars, layer, part, rate, prev_param, prev_layer, final):
    shape = p.shape[-2:]
    steps = 4
    count = len(nears)
    param_spec, layer_spec, wire_specs = chunk_specs(shape, layer, part, count, steps)
    args = [par, p, grad, col, *nears, *fars]
    in_specs = [pl.BlockSpec(memory_space=pltpu.SMEM), param_spec, layer_spec, layer_spec, *wire_specs, *wire_specs]
    aliases = {}
    out_shape = [jax.ShapeDtypeStruct(p.shape, F32)]
    out_specs = [param_spec]
    if not final:
        out_shape += [jax.ShapeDtypeStruct(shape, BF16)]
        out_shape += [jax.ShapeDtypeStruct((shape[0] // CHUNKS, shape[1]), BF16)] * count
        out_specs += [layer_spec, *wire_specs]
    n_prev = 0
    for prev, out_idx in ((prev_param, 0), (None if final else prev_layer, 1)):
        if prev is not None:
            aliases[len(args)] = out_idx
            args.append(prev)
            in_specs.append(ANY)
            n_prev += 1
    return pl.pallas_call(
        functools.partial(mix_kernel, rate, count, steps, n_prev, final),
        grid=(count * steps,),
        in_specs=in_specs, out_specs=out_specs, out_shape=out_shape,
        input_output_aliases=aliases,
        compiler_params=params_of(),
        cost_estimate=pl.CostEstimate(flops=10 ** 9, bytes_accessed=20 * count * shape[0] * shape[1] // CHUNKS,
                                      transcendentals=0),
    )(*args)


CAST_GROUPS = (1, 3, 4, 4, 4)
MIX_GROUPS = (2,) * 8
LAST_GROUPS = (2,) * 6 + (1,) * 4


def grouped(groups):
    first, out = 0, []
    for count in groups:
        out.append((first, count))
        first += count
    return out


def solution(mesh):
    row_size = mesh.shape["row"]
    col_size = mesh.shape["col"]
    layers, windows = 2, 2
    near_pairs = [(i, i ^ 1) for i in range(row_size)]
    far_pairs = [(i, i ^ 2) for i in range(row_size)]
    col_pairs = [(i, (i + 1) % col_size) for i in range(col_size)]

    def locate(i):
        return i // (2 * CHUNKS), (i // CHUNKS) % 2, i % CHUNKS

    def device_program(w_in, w_out, inputs, targets):
        batch, depth = inputs.shape[-2:]
        scale = 2.0 / (batch * depth)
        rate = LR_SCALE / layers
        par = (lax.axis_index("row") % 2).astype(jnp.int32).reshape(1)

        def send(i, wire, weights):
            near = lax.ppermute(wire, "row", near_pairs)
            far = lax.ppermute(near, "row", far_pairs)
            cols = None
            if i % CHUNKS == CHUNKS - 1:
                layer, kind, _ = locate(i)
                cols = lax.ppermute(weights[layer][kind], "col", col_pairs)
            return near, far, cols

        def fwd(layer, h, weights, t):
            w1, w2 = weights[layer]
            at = t if layer == 0 else None
            act, slope, ut = activate(h, at, w1)
            outs = hidden(act, w2, h, at, targets if layer == layers - 1 else None, t, scale)
            return (act, slope, ut, *outs)

        def run_forward(weights, t):
            outs, h = [], inputs
            for layer in range(layers):
                outs.append(fwd(layer, h, weights, t))
                h = outs[-1][3]
            return outs

        def grads(step, outs, weights, t, olds):
            g = outs[-1][4]
            found = [None] * layers
            for layer in reversed(range(layers)):
                act, slope, ut = outs[layer][:3]
                deep = (outs[layer - 1][3], outs[layer][3], targets) if layer else None
                res = None
                for part in range(PARTS[layer]):
                    res = backward(part, g, ut, act, slope,
                                 *weights[layer], *olds[layer], res, step == 1, rate, layer, deep, scale, t)
                if layer:
                    g = res[-1]
                found[layer] = res
            return found

        params = [w_in, w_out]
        weights = [[None, None] for _ in range(layers)]
        moved = []
        for first, count in grouped(CAST_GROUPS):
            layer, kind, part = locate(first)
            weights[layer][kind], *wires = cast_chunks(params[kind], layer, part, count,
                                                  weights[layer][kind])
            moved += [send(first + m, wire, weights) for m, wire in enumerate(wires)]
        head = run_forward(weights, 0)
        for window in range(windows):
            final = window == windows - 1
            step_a = 2 * window
            first = grads(0, head, weights, step_a, [params] * layers)
            moved_on = [r[2:4] for r in first]
            middle = run_forward(moved_on, step_a + 1)
            second = grads(1, middle, moved_on, step_a + 1, [r[:2] for r in first])
            new_params = [None, None]
            new_weights = [[None, None] for _ in range(layers)]
            new_moved, head = [], []
            for i, count in grouped(LAST_GROUPS if final else MIX_GROUPS):
                layer, kind, part = locate(i)
                members = moved[i:i + count]
                cols = moved[i - i % CHUNKS + CHUNKS - 1][2]
                res = mix_chunks(par, params[kind], second[layer][kind], cols,
                             [m[0] for m in members], [m[1] for m in members],
                             layer, part, rate, new_params[kind], new_weights[layer][kind], final)
                new_params[kind] = res[0]
                if not final:
                    new_weights[layer][kind] = res[1]
                    new_moved += [send(i + m, wire, new_weights) for m, wire in enumerate(res[2:])]
                    if (i + count) % (2 * CHUNKS) == 0:
                        h = inputs if layer == 0 else head[-1][3]
                        head.append(fwd(layer, h, new_weights, step_a + 2))
            params, weights, moved = new_params, new_weights, new_moved
        return params[0], params[1]

    block_spec = P("row", "col")
    return jax.shard_map(device_program, mesh=mesh, in_specs=(block_spec,) * 4, out_specs=(block_spec,) * 2, check_vma=False)
```

```python
import functools

import jax
import jax.numpy as jnp
from jax import lax
from jax.experimental import pallas as pl
from jax.experimental.pallas import tpu as pltpu
from jax.sharding import PartitionSpec as P


LR_SCALE = 0.8
EPS = 1e-6
INV_SQRT2 = 0.7071067811865476
INV_SQRT_2PI = 0.3989422804014327
HALF_LOG2E = -0.7213475204444817
F32 = jnp.float32
BF16 = jnp.bfloat16
CONTRACT_ROWS = (((0,), (0,)), ((), ()))
CONTRACT_LAST = (((1,), (1,)), ((), ()))
VMEM_LIMIT = 63 * 1024 * 1024
TILE = 512
ACT_TILE = 128
SLAB = 256
FWD_BLOCK = 512
BWD_BLOCK = 256
HID_TILE = 256
SPLIT = ((0, 0), (0, 1), (1, 1))
CHUNKS = 4
ANY = pl.BlockSpec(memory_space=pl.ANY)


def params_of(axes=1, limit=VMEM_LIMIT):
    return pltpu.CompilerParams(dimension_semantics=("arbitrary",) * axes, vmem_limit_bytes=limit)


def inv_rms_of(rows):
    return lax.rsqrt(jnp.mean(rows * rows, axis=-1, keepdims=True) + EPS)


def slabs(count, body):
    lax.fori_loop(0, count, lambda i, c: (body(pl.ds(pl.multiple_of(i * SLAB, SLAB), SLAB)), c)[1], 0)


def act_kernel(t, h_hbm, w1_ref, act_ref, slope_ref, ut_hbm, h_s, u_s, ut_s, z_s, sem, h_sems):
    step = pl.program_id(0)
    rows_total = h_s.shape[0]
    ut_copy = pltpu.make_async_copy(ut_s, ut_hbm, sem)
    h_rows = h_hbm if t is None else h_hbm.at[0, 0, t]

    def load(i):
        rows = pl.ds(pl.multiple_of(i * SLAB, SLAB), SLAB)
        return pltpu.make_async_copy(h_rows.at[rows], h_s.at[rows], h_sems.at[i])

    @pl.when(step == 0)
    def _():
        for i in range(rows_total // SLAB):
            load(i).start()

        def normalize(i, carry):
            rows = pl.ds(pl.multiple_of(i * SLAB, SLAB), SLAB)
            load(i).wait()
            h = h_s[rows, :].astype(F32)
            u = h * inv_rms_of(h)
            u_s[rows, :] = u.astype(BF16)
            ut_s[:, rows] = u.T.astype(BF16)
            return carry

        lax.fori_loop(0, rows_total // SLAB, normalize, 0)
        ut_copy.start()

    for i in range(rows_total // ACT_TILE):
        rows = pl.ds(i * ACT_TILE, ACT_TILE)
        z = z_s[rows, :]
        half = 0.5 * (1.0 + lax.erf(z * INV_SQRT2))
        act_ref[rows, :] = (z * half).astype(BF16)
        slope_ref[rows, :] = half + (z * INV_SQRT_2PI) * jnp.exp2(z * z * HALF_LOG2E)
        z_s[rows, :] = jnp.dot(u_s[rows, :], w1_ref[...], preferred_element_type=F32)

    @pl.when(step == pl.num_programs(0) - 1)
    def _():
        ut_copy.wait()


def activate(h, t, w1):
    depth, ff = w1.shape
    rows = h.shape[-2]
    block = FWD_BLOCK
    blocks = ff // block
    done_block = pl.BlockSpec((rows, block), lambda j: (0, jnp.maximum(j - 1, 0)))
    return pl.pallas_call(
        functools.partial(act_kernel, t),
        grid=(blocks + 1,),
        in_specs=[ANY, pl.BlockSpec((depth, block), lambda j: (0, jnp.minimum(j, blocks - 1)))],
        out_specs=[done_block, done_block, ANY],
        out_shape=[jax.ShapeDtypeStruct((rows, ff), BF16), jax.ShapeDtypeStruct((rows, ff), F32),
                   jax.ShapeDtypeStruct((depth, rows), BF16)],
        scratch_shapes=[pltpu.VMEM((rows, depth), BF16), pltpu.VMEM((rows, depth), BF16), pltpu.VMEM((depth, rows), BF16),
                        pltpu.VMEM((rows, block), F32), pltpu.SemaphoreType.DMA, pltpu.SemaphoreType.DMA((rows // SLAB,))],
        compiler_params=params_of(),
        cost_estimate=pl.CostEstimate(flops=2 * rows * depth * ff, bytes_accessed=rows * ff * 6 + depth * ff * 2,
                                      transcendentals=2 * rows * ff),
    )(h, w1)


def hidden_kernel(last, scale, act_ref, w2_hbm, h_ref, *refs):
    *refs, w2_s, add_s, sems = refs
    step = pl.program_id(0)
    bands = 4
    band = w2_s.shape[0] // bands

    @pl.when(step == 0)
    def _():
        pieces = [pl.ds(i * band, band) for i in range(bands)]
        loads = [pltpu.make_async_copy(w2_hbm.at[piece], w2_s.at[piece], sems.at[i]) for i, piece in enumerate(pieces)]
        for load in loads:
            load.start()
        for i, (piece, load) in enumerate(zip(pieces, loads)):
            load.wait()
            add = jnp.dot(act_ref[:, piece], w2_s[piece, :], preferred_element_type=F32)
            add_s[...] = add_s[...] + add if i else add

    @pl.when(step > 0)
    def _():
        add_s[...] = jnp.dot(act_ref[...], w2_s[...], preferred_element_type=F32)

    h = (h_ref[...].astype(F32) + add_s[...]).astype(BF16)
    if last:
        tgt_ref, hout_ref, g_ref = refs
        g_ref[...] = ((h.astype(F32) - tgt_ref[...].astype(F32)) * scale).astype(BF16)
    else:
        hout_ref, = refs
    hout_ref[...] = h


def hidden(act, w2, h, t, target, target_t, scale):
    ff, depth = w2.shape
    rows = act.shape[0]
    tile = HID_TILE
    plain = pl.BlockSpec((tile, depth), lambda i: (i, 0))
    of_step = lambda t: pl.BlockSpec((None, None, None, tile, depth), lambda i: (0, 0, t, i, 0))
    last = target is not None
    n_out = 2 if last else 1
    return pl.pallas_call(
        functools.partial(hidden_kernel, last, scale),
        grid=(rows // tile,),
        in_specs=[pl.BlockSpec((tile, ff), lambda i: (i, 0)),
                  ANY,
                  plain if t is None else of_step(t)] + ([of_step(target_t)] if last else []),
        out_specs=[plain] * n_out,
        out_shape=[jax.ShapeDtypeStruct((rows, depth), BF16)] * n_out,
        scratch_shapes=[pltpu.VMEM((ff, depth), BF16), pltpu.VMEM((tile, depth), F32), pltpu.SemaphoreType.DMA((4,))],
        compiler_params=params_of(),
        cost_estimate=pl.CostEstimate(flops=2 * rows * depth * ff, bytes_accessed=rows * ff * 2 + depth * ff * 2,
                                      transcendentals=0),
    )(act, w2, h, *([target] if last else []))


def parts_of(window, step, layer):
    return 2 if layer or (window, step) in SPLIT else 1


def bwd_kernel(deep, second, part, parts, scale, rate, t, n_prev, *refs):
    refs = list(refs)

    def take(count):
        taken = refs[:count]
        del refs[:count]
        return taken

    g_ref, ut_ref, act_ref, slope_ref, w2_ref = take(5)
    closing = deep and part == parts - 1
    if deep:
        w1_ref, = take(1)
    if deep and part:
        acc_in_hbm, = take(1)
    if closing:
        h_hbm, hl_hbm, tgt_hbm = take(3)
    old1_ref, old2_ref = take(2)
    take(n_prev)
    d1_ref, d2_ref = take(2)
    if not second:
        q1_ref, q2_ref = take(2)
    if deep:
        out_hbm, = take(1)
    s_s, = take(1)
    if deep:
        acc, sems = take(2)
    if closing:
        h_s, hl_s, tgt_s, gout_s = take(4)
    step = pl.program_id(0)
    rows_total = g_ref.shape[0]
    if deep:
        @pl.when(step == 0)
        def _():
            if part:
                acc_load = pltpu.make_async_copy(acc_in_hbm, acc, sems.at[0])
                acc_load.start()
                acc_load.wait()
            else:
                def clear(rows):
                    acc[rows, :] = jnp.zeros((SLAB, acc.shape[1]), F32)

                slabs(rows_total // SLAB, clear)
    if closing:
        loads = [pltpu.make_async_copy(src, dst, sems.at[i + 1])
                 for i, (src, dst) in enumerate(((h_hbm, h_s), (hl_hbm, hl_s), (tgt_hbm.at[0, 0, t], tgt_s)))]

        for i, load in enumerate(loads):
            pl.when(step == i + 2)(load.start)

    for i in range(rows_total // TILE):
        rows = pl.ds(i * TILE, TILE)
        back = lax.dot_general(g_ref[rows, :], w2_ref[...], CONTRACT_LAST, preferred_element_type=F32)
        s_s[rows, :] = (back * slope_ref[rows, :]).astype(BF16)

    d2 = lax.dot_general(act_ref[...], g_ref[...], CONTRACT_ROWS, preferred_element_type=F32)
    d1 = jnp.dot(ut_ref[...], s_s[...], preferred_element_type=F32)
    if second:
        d2_ref[...] = old2_ref[...] + d2
        d1_ref[...] = old1_ref[...] + d1
    else:
        d2_ref[...] = d2
        d1_ref[...] = d1
        q2_ref[...] = (old2_ref[...] - rate * d2).astype(BF16)
        q1_ref[...] = (old1_ref[...] - rate * d1).astype(BF16)
    if deep:
        for i in range(rows_total // TILE):
            rows = pl.ds(i * TILE, TILE)
            acc[rows, :] += lax.dot_general(s_s[rows, :], w1_ref[...], CONTRACT_LAST, preferred_element_type=F32)

        @pl.when(step == pl.num_programs(0) - 1)
        def _():
            out_copy = pltpu.make_async_copy(gout_s if closing else acc, out_hbm, sems.at[0])
            if closing:
                for load in loads:
                    load.wait()

                def finish(rows):
                    h = h_s[rows, :].astype(F32)
                    grad = acc[rows, :]
                    inv_rms = inv_rms_of(h)
                    row_dot = jnp.mean(h * grad, axis=-1, keepdims=True)
                    e = (hl_s[rows, :].astype(F32) - tgt_s[rows, :].astype(F32)) * scale
                    e = e + (inv_rms * grad - h * (inv_rms * inv_rms * inv_rms) * row_dot)
                    gout_s[rows, :] = e.astype(BF16)

                slabs(rows_total // SLAB, finish)
            out_copy.start()
            out_copy.wait()


def backward(part, parts, g, ut, act, slope, w1, w2, old1, old2, prev, second, rate, layer, deep, scale, t):
    rows, ff = act.shape
    depth = g.shape[1]
    is_deep = deep is not None
    closing = is_deep and part == parts - 1
    block = BWD_BLOCK
    steps = ff // block // parts
    first = part * steps
    in_cols = pl.BlockSpec((depth, block), lambda j: (0, first + j))
    out_rows = pl.BlockSpec((block, depth), lambda j: (first + j, 0))
    wide = pl.BlockSpec((rows, block), lambda j: (0, first + j))
    if second:
        old_specs = [in_cols, out_rows]
    else:
        old_specs = [pl.BlockSpec((None, None, None, depth, block), lambda j: (0, 0, layer, 0, first + j)),
                     pl.BlockSpec((None, None, None, block, depth), lambda j: (0, 0, layer, first + j, 0))]
    once = pl.Buffered(1)
    args = [g, ut, act, slope, w2]
    in_specs = [pl.BlockSpec((rows, depth), lambda j: (0, 0), pipeline_mode=once),
                pl.BlockSpec((depth, rows), lambda j: (0, 0), pipeline_mode=once), wide, wide, out_rows]
    n_grads = 2 if second else 4
    if is_deep:
        args.append(w1)
        in_specs.append(in_cols)
    if is_deep and part:
        args.append(prev[-1])
        in_specs.append(ANY)
    if closing:
        args += list(deep)
        in_specs += [ANY] * 3
    args += [old1, old2]
    in_specs += old_specs
    aliases, n_prev = {}, 0
    if part:
        n_prev = n_grads
        for i in range(n_grads):
            aliases[len(args)] = i
            args.append(prev[i])
            in_specs.append(ANY)
    out_shape = [jax.ShapeDtypeStruct((depth, ff), F32), jax.ShapeDtypeStruct((ff, depth), F32)]
    out_specs = [in_cols, out_rows]
    if not second:
        out_shape += [jax.ShapeDtypeStruct((depth, ff), BF16), jax.ShapeDtypeStruct((ff, depth), BF16)]
        out_specs += [in_cols, out_rows]
    scratch = [pltpu.VMEM((rows, block), BF16)]
    if is_deep:
        out_shape.append(jax.ShapeDtypeStruct((rows, depth), BF16 if closing else F32))
        out_specs.append(ANY)
        scratch += [pltpu.VMEM((rows, depth), F32), pltpu.SemaphoreType.DMA((4,))]
    if closing:
        scratch += [pltpu.VMEM((rows, depth), BF16)] * 4
    return pl.pallas_call(
        functools.partial(bwd_kernel, is_deep, second, part, parts, scale, rate, t, n_prev),
        grid=(steps,),
        in_specs=in_specs, out_specs=out_specs, out_shape=out_shape, scratch_shapes=scratch,
        input_output_aliases=aliases,
        compiler_params=params_of(),
        cost_estimate=pl.CostEstimate(flops=(8 if is_deep else 6) * rows * depth * ff // parts,
                                      bytes_accessed=(rows * ff * 6 + depth * ff * 24) // parts, transcendentals=0),
    )(*args)


def chunk_specs(shape, layer, part, count, steps):
    rows, cols = shape
    band = rows // CHUNKS // steps
    first = part * steps

    def alone(m):
        return pl.BlockSpec((band, cols), lambda j: (jnp.clip(j - m * steps, 0, steps - 1), 0))

    return (pl.BlockSpec((None, None, None, band, cols), lambda j: (0, 0, layer, first + j, 0)),
            pl.BlockSpec((band, cols), lambda j: (first + j, 0)),
            [alone(m) for m in range(count)])


def in_turn(count, steps, body):
    if count == 1:
        return body(0)
    turn = pl.program_id(0) // steps
    for m in range(count):
        pl.when(turn == m)(functools.partial(body, m))


def cast_kernel(count, steps, n_prev, p_ref, *refs):
    whole_ref, *wire_refs = refs[n_prev:]
    value = p_ref[...].astype(BF16)
    whole_ref[...] = value

    def put(m):
        wire_refs[m][...] = value

    in_turn(count, steps, put)


def cast_chunks(p, layer, part, count, prev):
    shape = p.shape[-2:]
    steps = 2
    param_spec, layer_spec, wire_specs = chunk_specs(shape, layer, part, count, steps)
    args, in_specs = [p], [param_spec]
    if prev is not None:
        args.append(prev)
        in_specs.append(ANY)
    wire = jax.ShapeDtypeStruct((shape[0] // CHUNKS, shape[1]), BF16)
    return pl.pallas_call(
        functools.partial(cast_kernel, count, steps, len(args) - 1),
        grid=(count * steps,),
        in_specs=in_specs,
        out_specs=[layer_spec, *wire_specs],
        out_shape=[jax.ShapeDtypeStruct(shape, BF16)] + [wire] * count,
        input_output_aliases={1: 0} if prev is not None else {},
        compiler_params=params_of(),
        cost_estimate=pl.CostEstimate(flops=10 ** 9, bytes_accessed=8 * count * shape[0] * shape[1] // CHUNKS,
                                      transcendentals=0),
    )(*args)


def mix_kernel(rate, count, steps, n_prev, final, par_ref, p_ref, grad_ref, col_ref, *refs):
    near_refs, far_refs = refs[:count], refs[count:2 * count]
    outs = refs[2 * count + n_prev:]
    even = par_ref[0] == 0

    def mix_one(m):
        near = near_refs[m][...].astype(F32)
        far = far_refs[m][...].astype(F32)
        col = col_ref[...].astype(F32)
        mix = p_ref[...] + col + col
        mix = mix + jnp.where(even, far, near)
        mix = mix + jnp.where(even, near, far)
        new = mix / 5.0 - rate * grad_ref[...]
        outs[0][...] = new
        if not final:
            value = new.astype(BF16)
            outs[1][...] = value
            outs[2 + m][...] = value

    in_turn(count, steps, mix_one)


def mix_chunks(par, p, grad, col, nears, fars, layer, part, rate, prev_param, prev_layer, final):
    shape = p.shape[-2:]
    steps = 4
    count = len(nears)
    param_spec, layer_spec, wire_specs = chunk_specs(shape, layer, part, count, steps)
    args = [par, p, grad, col, *nears, *fars]
    in_specs = [pl.BlockSpec(memory_space=pltpu.SMEM), param_spec, layer_spec, layer_spec, *wire_specs, *wire_specs]
    aliases = {}
    out_shape = [jax.ShapeDtypeStruct(p.shape, F32)]
    out_specs = [param_spec]
    if not final:
        out_shape += [jax.ShapeDtypeStruct(shape, BF16)]
        out_shape += [jax.ShapeDtypeStruct((shape[0] // CHUNKS, shape[1]), BF16)] * count
        out_specs += [layer_spec, *wire_specs]
    n_prev = 0
    for prev, out_idx in ((prev_param, 0), (None if final else prev_layer, 1)):
        if prev is not None:
            aliases[len(args)] = out_idx
            args.append(prev)
            in_specs.append(ANY)
            n_prev += 1
    return pl.pallas_call(
        functools.partial(mix_kernel, rate, count, steps, n_prev, final),
        grid=(count * steps,),
        in_specs=in_specs, out_specs=out_specs, out_shape=out_shape,
        input_output_aliases=aliases,
        compiler_params=params_of(),
        cost_estimate=pl.CostEstimate(flops=10 ** 9, bytes_accessed=20 * count * shape[0] * shape[1] // CHUNKS,
                                      transcendentals=0),
    )(*args)


CAST_GROUPS = (1, 3, 4, 4, 1, 3)
MIX_GROUPS = (4, 4, 4, 2, 2)
LAST_GROUPS = (4, 4, 4, 1, 1, 1, 1)


def grouped(groups):
    first, out = 0, []
    for count in groups:
        out.append((first, count))
        first += count
    return out


def solution(mesh):
    row_size = mesh.shape["row"]
    col_size = mesh.shape["col"]
    layers, windows = 2, 2
    near_pairs = [(i, i ^ 1) for i in range(row_size)]
    far_pairs = [(i, i ^ 2) for i in range(row_size)]
    col_pairs = [(i, (i + 1) % col_size) for i in range(col_size)]

    def locate(i):
        return i // (2 * CHUNKS), (i // CHUNKS) % 2, i % CHUNKS

    def device_program(w_in, w_out, inputs, targets):
        batch, depth = inputs.shape[-2:]
        scale = 2.0 / (batch * depth)
        rate = LR_SCALE / layers
        par = (lax.axis_index("row") % 2).astype(jnp.int32).reshape(1)

        def send(i, wire, weights):
            near = lax.ppermute(wire, "row", near_pairs)
            far = lax.ppermute(near, "row", far_pairs)
            cols = None
            if i % CHUNKS == CHUNKS - 1:
                layer, kind, _ = locate(i)
                cols = lax.ppermute(weights[layer][kind], "col", col_pairs)
            return near, far, cols

        def fwd(layer, h, weights, t):
            w1, w2 = weights[layer]
            at = t if layer == 0 else None
            act, slope, ut = activate(h, at, w1)
            outs = hidden(act, w2, h, at, targets if layer == layers - 1 else None, t, scale)
            return (act, slope, ut, *outs)

        def run_forward(weights, t):
            outs, h = [], inputs
            for layer in range(layers):
                outs.append(fwd(layer, h, weights, t))
                h = outs[-1][3]
            return outs

        def grads(window, step, outs, weights, t, olds):
            g = outs[-1][4]
            found = [None] * layers
            for layer in reversed(range(layers)):
                act, slope, ut = outs[layer][:3]
                deep = (outs[layer - 1][3], outs[layer][3], targets) if layer else None
                res = None
                parts = parts_of(window, step, layer)
                for part in range(parts):
                    res = backward(part, parts, g, ut, act, slope,
                                 *weights[layer], *olds[layer], res, step == 1, rate, layer, deep, scale, t)
                if layer:
                    g = res[-1]
                found[layer] = res
            return found

        params = [w_in, w_out]
        weights = [[None, None] for _ in range(layers)]
        moved = []
        for first, count in grouped(CAST_GROUPS):
            layer, kind, part = locate(first)
            weights[layer][kind], *wires = cast_chunks(params[kind], layer, part, count,
                                                  weights[layer][kind])
            moved += [send(first + m, wire, weights) for m, wire in enumerate(wires)]
        head = run_forward(weights, 0)
        for window in range(windows):
            final = window == windows - 1
            step_a = 2 * window
            first = grads(window, 0, head, weights, step_a, [params] * layers)
            moved_on = [r[2:4] for r in first]
            middle = run_forward(moved_on, step_a + 1)
            second = grads(window, 1, middle, moved_on, step_a + 1, [r[:2] for r in first])
            new_params = [None, None]
            new_weights = [[None, None] for _ in range(layers)]
            new_moved, head = [], []
            for i, count in grouped(LAST_GROUPS if final else MIX_GROUPS):
                layer, kind, part = locate(i)
                members = moved[i:i + count]
                cols = moved[i - i % CHUNKS + CHUNKS - 1][2]
                res = mix_chunks(par, params[kind], second[layer][kind], cols,
                             [m[0] for m in members], [m[1] for m in members],
                             layer, part, rate, new_params[kind], new_weights[layer][kind], final)
                new_params[kind] = res[0]
                if not final:
                    new_weights[layer][kind] = res[1]
                    new_moved += [send(i + m, wire, new_weights) for m, wire in enumerate(res[2:])]
                    if (i + count) % (2 * CHUNKS) == 0:
                        h = inputs if layer == 0 else head[-1][3]
                        head.append(fwd(layer, h, new_weights, step_a + 2))
            params, weights, moved = new_params, new_weights, new_moved
        return params[0], params[1]

    block_spec = P("row", "col")
    return jax.shard_map(device_program, mesh=mesh, in_specs=(block_spec,) * 4, out_specs=(block_spec,) * 2, check_vma=False)
```
